16 devices in a mesh: dp: 2 (over y, z), tp: 8 (over x, core).
Axes of the slice: x: 4, y: 2, z: 1, core: 2. Of those that a mesh axis runs over, the one named last changes fastest.
The devices are a block of a 4x4x8 slice.
Arguments:
- X: bfloat16 [512, 4096], P(('dp', 'tp')), parts along dimension 0
- dY: bfloat16 [512, 4096], P(('dp', 'tp')), parts along dimension 0
- W1: bfloat16 [4096, 14336], P(None, 'tp')
- W2: bfloat16 [14336, 4096], P('tp')
Outputs:
- output 1: bfloat16 [512, 4096], P(('dp', 'tp')), parts along dimension 0
- output 2: float32 [8192, 14336], P('dp', 'tp'), parts along dimension 0
- output 3: float32 [28672, 4096], P(('dp', 'tp')), parts along dimension 0
There are 2 independent parts. The reference program is written for one: setup_inputs(seed, part) draws one part's arguments, and reference() takes and returns one part's arrays. A program takes and returns all parts, laid end to end along the dimension named above; an argument that names none is the same for every part.
All inputs are finite; a program needn't handle non-finite values.
Results may differ from the reference program's by a relative error of at most 0.00941025.
Values are sent between devices in bfloat16 or wider.
A program may use at most 768 MiB of HBM per device.

```python
import math
import jax
import jax.numpy as jnp
from jax import lax

TP = 8
TOKENS_DEV = 32
H = 4096
FF_DEV = 1792

T = TOKENS_DEV * TP
F = FF_DEV * TP
C0 = math.sqrt(2.0 / math.pi)
C1 = 0.044715


def _gelu(u):
    t = jnp.tanh(C0 * (u + C1 * u * u * u))
    return 0.5 * u * (1.0 + t), 0.5 * (1.0 + t) + 0.5 * u * (1.0 - t * t) * C0 * (1.0 + 3.0 * C1 * u * u)


def setup_inputs(seed: int = 0, part: int = 0) -> dict:
    key = jax.random.PRNGKey(seed)
    ks = jax.random.split(key, 3)
    kx, kdy = jax.random.split(jax.random.fold_in(ks[0], part))
    x = jax.random.normal(kx, (T, H), jnp.float32).astype(jnp.bfloat16)
    dy = jax.random.normal(kdy, (T, H), jnp.float32).astype(jnp.bfloat16)
    w1 = (jax.random.normal(ks[1], (H, F), jnp.float32) * H ** -0.5).astype(jnp.bfloat16)
    w2 = (jax.random.normal(ks[2], (F, H), jnp.float32) * F ** -0.5).astype(jnp.bfloat16)
    return {'X': x, 'dY': dy, 'W1': w1, 'W2': w2}


def reference(X, dY, W1, W2):
    w1c = W1.reshape(H, TP, FF_DEV).transpose(1, 0, 2)
    w2c = W2.reshape(TP, FF_DEV, H)

    def step(acc, w):
        a, b = w
        u = jnp.dot(X, a, preferred_element_type=jnp.float32).astype(jnp.bfloat16)
        g0, g1 = _gelu(u.astype(jnp.float32))
        z = g0.astype(jnp.bfloat16)
        dw2 = jnp.dot(z.T, dY, preferred_element_type=jnp.float32)
        g = jnp.dot(dY, b.T, preferred_element_type=jnp.float32)
        dz = (g * g1).astype(jnp.bfloat16)
        acc = acc + jnp.dot(dz, a.T, preferred_element_type=jnp.float32)
        dw1 = jnp.dot(X.T, dz, preferred_element_type=jnp.float32)
        return acc, (dw1, dw2)

    acc, (dw1, dw2) = lax.scan(step, jnp.zeros((T, H), jnp.float32), (w1c, w2c))
    dX = acc.astype(jnp.bfloat16)
    dW1 = dw1.transpose(1, 0, 2).reshape(H, F)
    dW2 = dw2.reshape(F, H)
    return (dX, dW1, dW2)
```

```python
import functools
import math

import jax
import jax.numpy as jnp
from jax import lax
from jax.experimental import pallas as pl
from jax.experimental.pallas import tpu as pltpu
from jax.sharding import PartitionSpec as P

C0 = math.sqrt(2.0 / math.pi)
C1 = 0.044715
F32 = jnp.float32
BF16 = jnp.bfloat16
NQ = 4
LEAD = 3
NT = (((1,), (1,)), ((), ()))
TN = (((0,), (0,)), ((), ()))


def _gelu(u):
    t = jnp.tanh(C0 * (u + C1 * u * u * u))
    return 0.5 * u * (1.0 + t), 0.5 * (1.0 + t) + 0.5 * u * (1.0 - t * t) * C0 * (1.0 + 3.0 * C1 * u * u)


def _forward_kernel(ntp, x, dy, w1, w2, g_o, z_o, dz_o, r0_o, r1_o, r2_o, r3_o,
                    g, w1v, w2v, acc, dact, z, dz, part, sendb, recvb, r0, rr,
                    lsem, wsem, osem, ssem, rsem, psem):
    nchip = ntp // 2
    rows, h = x.shape
    hc = h // NQ
    f = w1.shape[1]
    me = lax.axis_index('tp')
    c = lax.rem(me, 2)
    chip = me // 2
    partner = me + 1 - 2 * c
    right = lax.rem(chip + 1, nchip) * 2 + c
    left = lax.rem(chip + nchip - 1, nchip) * 2 + c
    opp = lax.rem(chip + 2, nchip) * 2 + c
    fsrc = left * (1 - c) + right * c
    fdst = right * (1 - c) + left * c
    flip = 1 - 2 * c

    def piece(q, dev):
        return g.at[q, pl.ds(pl.multiple_of(dev * rows, rows), rows), :]

    def rcopy(q, slot, dev, to):
        return pltpu.make_async_remote_copy(
            src_ref=piece(q, dev), dst_ref=piece(q, dev), send_sem=ssem.at[q, slot], recv_sem=rsem.at[q, slot],
            device_id={'tp': to}, device_id_type=pl.DeviceIdType.MESH)

    own = []
    for q in range(2 * NQ):
        src = x if q < NQ else dy
        cp = pltpu.make_async_copy(src.at[:, pl.ds((q % NQ) * hc, hc)], piece(q, me), lsem.at[q])
        cp.start()
        own.append(cp)
    wcp = []
    for q in range(NQ):
        cp = pltpu.make_async_copy(w1.at[pl.ds(q * hc, hc), :], w1v.at[pl.ds(q * hc, hc), :], wsem.at[q])
        cp.start()
        wcp.append(cp)
    for q in range(NQ):
        cp = pltpu.make_async_copy(w2.at[:, pl.ds(q * hc, hc)], w2v.at[q], wsem.at[NQ + q])
        cp.start()
        wcp.append(cp)

    barrier = pltpu.get_barrier_semaphore()
    for nb in (partner, right, left):
        pl.semaphore_signal(barrier, inc=1, device_id={'tp': nb}, device_id_type=pl.DeviceIdType.MESH)
    pl.semaphore_wait(barrier, 3)

    started = []

    def send(q, slot, dev, to):
        cp = rcopy(q, slot, dev, to)
        cp.start()
        started.append(cp)

    def send_own(q):
        own[q].wait()
        send(q, 0, me, right)
        send(q, 1, me, left)
        send(q, 3, me, partner)

    def hop(q):
        rcopy(q, 0, left, me + 0).wait_recv()
        rcopy(q, 1, right, me + 0).wait_recv()
        send(q, 2, fsrc, fdst)
        send(q, 4, left, partner)
        send(q, 5, right, partner)

    def last(q):
        rcopy(q, 2, opp, me + 0).wait_recv()
        send(q, 6, opp, partner)

    def arrived(q):
        rcopy(q, 3, partner, me + 0).wait_recv()
        rcopy(q, 4, left + flip, me + 0).wait_recv()
        rcopy(q, 5, right + flip, me + 0).wait_recv()
        rcopy(q, 6, opp + flip, me + 0).wait_recv()

    outs = []

    def put(src, dst):
        cp = pltpu.make_async_copy(src, dst, osem.at[len(outs)])
        cp.start()
        outs.append(cp)

    def compute(q):
        if q < NQ:
            wcp[q].wait()
            p = jnp.dot(g[q], w1v[pl.ds(q * hc, hc), :], preferred_element_type=F32)
        else:
            wcp[q].wait()
            p = lax.dot_general(g[q], w2v[q - NQ], NT, preferred_element_type=F32)
        if q % NQ == 0:
            acc[...] = p
        else:
            acc[...] += p
        put(g.at[q], g_o.at[q])
        if q == NQ - 1:
            @pl.loop(0, f // 256)
            def _(i):
                cols = pl.ds(pl.multiple_of(i * 256, 256), 256)
                g0, g1 = _gelu(acc[:, cols].astype(BF16).astype(F32))
                z[:, cols] = g0.astype(BF16)
                dact[:, cols] = g1
            put(z, z_o)

    for q in range(LEAD):
        send_own(q)
    for s in range(2 * NQ + 2):
        if s < 2 * NQ:
            hop(s)
            if s + LEAD < 2 * NQ:
                send_own(s + LEAD)
        if 0 <= s - 1 < 2 * NQ:
            last(s - 1)
        if 0 <= s - 2 < 2 * NQ:
            arrived(s - 2)
            compute(s - 2)

    dz[...] = (acc[...] * dact[...]).astype(BF16)
    put(dz, dz_o)

    def pair(j):
        return pltpu.make_async_remote_copy(
            src_ref=sendb.at[j], dst_ref=recvb.at[j], send_sem=psem.at[0, j], recv_sem=psem.at[1, j],
            device_id={'tp': partner}, device_id_type=pl.DeviceIdType.MESH)

    def block(d, core):
        dest = lax.rem(chip + d, nchip) * 2 + core
        return pl.ds(pl.multiple_of(dest * rows, rows), rows)

    def combine(j):
        pair(j).wait_recv()
        cols = pl.ds(j * hc, hc)
        for d in range(nchip):
            s = part[j % 2, block(d, c), :] + recvb[j, d].astype(F32)
            if d == 0:
                r0[:, cols] = s
            else:
                rr[d - 1, :, cols] = s.astype(BF16)

    for j in range(NQ):
        part[j % 2] = lax.dot_general(dz[...], w1v[pl.ds(j * hc, hc), :], NT, preferred_element_type=F32)
        for d in range(nchip):
            sendb[j, d] = part[j % 2, block(d, 1 - c), :].astype(BF16)
        cp = pair(j)
        cp.start()
        started.append(cp)
        if j > 0:
            combine(j - 1)
    combine(NQ - 1)
    put(r0, r0_o)
    for d, o in enumerate((r1_o, r2_o, r3_o)):
        put(rr.at[d], o)
    for cp in started:
        cp.wait_send()
    for cp in outs:
        cp.wait()


def _weight_grad_kernel(g, z, dz, dw1, dw2, ga, za, dza, b1, b2, isem, sem1, sem2):
    nq, t, hc = g.shape[0] // 2, g.shape[1], g.shape[2]
    f = z.shape[1]
    n1, n2 = b1.shape[0], b2.shape[0]
    t1, t2 = b1.shape[1], b2.shape[1]
    k1, k2 = nq * hc // t1, f // t2
    cz = pltpu.make_async_copy(z, za, isem.at[0])
    cy = pltpu.make_async_copy(g.at[pl.ds(nq, nq)], ga.at[pl.ds(nq, nq)], isem.at[1])
    cx = pltpu.make_async_copy(g.at[pl.ds(0, nq)], ga.at[pl.ds(0, nq)], isem.at[2])
    cd = pltpu.make_async_copy(dz, dza, isem.at[3])
    for cp in (cz, cy, cd, cx):
        cp.start()
    cz.wait()
    cy.wait()

    def out2(i):
        s = lax.rem(i, n2)
        return pltpu.make_async_copy(b2.at[s], dw2.at[pl.ds(pl.multiple_of(i * t2, t2), t2), :], sem2.at[s])

    def out1(i):
        s = lax.rem(i, n1)
        return pltpu.make_async_copy(b1.at[s], dw1.at[pl.ds(pl.multiple_of(i * t1, t1), t1), :], sem1.at[s])

    @pl.loop(0, k2)
    def _(i):
        @pl.when(i >= n2)
        def _():
            out2(i - n2).wait()
        zt = za[:, pl.ds(pl.multiple_of(i * t2, t2), t2)]
        s = lax.rem(i, n2)
        for q in range(nq):
            b2[s, :, pl.ds(q * hc, hc)] = lax.dot_general(zt, ga[nq + q], TN, preferred_element_type=F32)
        out2(i).start()

    cd.wait()
    cx.wait()
    per = hc // t1

    @pl.loop(0, k1)
    def _(i):
        @pl.when(i >= n1)
        def _():
            out1(i - n1).wait()
        xt = ga[i // per, :, pl.ds(pl.multiple_of(lax.rem(i, per) * t1, t1), t1)]
        b1[lax.rem(i, n1)] = lax.dot_general(xt, dza[...], TN, preferred_element_type=F32)
        out1(i).start()

    for i in range(max(0, k2 - n2), k2):
        out2(i).wait()
    for i in range(max(0, k1 - n1), k1):
        out1(i).wait()


def solution(mesh):
    ntp = mesh.shape['tp']
    nchip = ntp // 2
    any_spec = pl.BlockSpec(memory_space=pl.ANY)

    def body(x, dy, w1, w2):
        rows, h = x.shape
        f = w1.shape[1]
        t, hc = rows * ntp, h // NQ
        sds = jax.ShapeDtypeStruct
        dma = pltpu.SemaphoreType.DMA
        g, z, dz, r0, r1, r2, r3 = pl.pallas_call(
            functools.partial(_forward_kernel, ntp),
            name='gather_forward',
            out_shape=[sds((2 * NQ, t, hc), BF16), sds((t, f), BF16), sds((t, f), BF16), sds((rows, h), F32),
                       sds((rows, h), BF16), sds((rows, h), BF16), sds((rows, h), BF16)],
            in_specs=[any_spec] * 4,
            out_specs=[any_spec] * 7,
            scratch_shapes=[
                pltpu.VMEM((2 * NQ, t, hc), BF16),
                pltpu.VMEM((h, f), BF16),
                pltpu.VMEM((NQ, f, hc), BF16),
                pltpu.VMEM((t, f), F32),
                pltpu.VMEM((t, f), F32),
                pltpu.VMEM((t, f), BF16),
                pltpu.VMEM((t, f), BF16),
                pltpu.VMEM((2, t, hc), F32),
                pltpu.VMEM((NQ, nchip, rows, hc), BF16),
                pltpu.VMEM((NQ, nchip, rows, hc), BF16),
                pltpu.VMEM((rows, h), F32),
                pltpu.VMEM((nchip - 1, rows, h), BF16),
                dma((2 * NQ,)), dma((2 * NQ,)), dma((2 * NQ + 6,)),
                dma((2 * NQ, 7)), dma((2 * NQ, 7)), dma((2, NQ)),
            ],
            compiler_params=pltpu.CompilerParams(
                collective_id=0, has_side_effects=True, vmem_limit_bytes=60 * 2 ** 20),
            cost_estimate=pl.CostEstimate(flops=6 * t * h * f, bytes_accessed=4 * h * f, transcendentals=t * f),
        )(x, dy, w1, w2)

        def ring(d):
            return [(2 * i + k, 2 * ((i + d) % nchip) + k) for i in range(nchip) for k in range(2)]

        p2 = lax.ppermute(r2, 'tp', ring(2))
        p1 = lax.ppermute(r1, 'tp', ring(1))
        p3 = lax.ppermute(r3, 'tp', ring(3))
        t1, t2 = 512, 256
        dw1, dw2 = pl.pallas_call(
            _weight_grad_kernel,
            name='weight_grads',
            out_shape=[sds((h, f), F32), sds((f, h), F32)],
            in_specs=[any_spec] * 3,
            out_specs=[any_spec] * 2,
            scratch_shapes=[
                pltpu.VMEM((2 * NQ, t, hc), BF16),
                pltpu.VMEM((t, f), BF16),
                pltpu.VMEM((t, f), BF16),
                pltpu.VMEM((4, t1, f), F32),
                pltpu.VMEM((4, t2, h), F32),
                dma((4,)), dma((4,)), dma((4,)),
            ],
            compiler_params=pltpu.CompilerParams(vmem_limit_bytes=48 * 2 ** 20),
            cost_estimate=pl.CostEstimate(flops=4 * t * h * f, bytes_accessed=8 * h * f, transcendentals=0),
        )(g, z, dz)
        dx = (r0 + p1.astype(F32) + p3.astype(F32) + p2.astype(F32)).astype(BF16)
        return dx, dw1, dw2

    return jax.shard_map(
        body, mesh=mesh,
        in_specs=(P(('dp', 'tp'), None), P(('dp', 'tp'), None), P(None, 'tp'), P('tp', None)),
        out_specs=(P(('dp', 'tp'), None), P('dp', 'tp'), P(('dp', 'tp'), None)),
        check_vma=False)
```

```python
import functools
import math

import jax
import jax.numpy as jnp
from jax import lax
from jax.experimental import pallas as pl
from jax.experimental.pallas import tpu as pltpu
from jax.sharding import PartitionSpec as P

C0 = math.sqrt(2.0 / math.pi)
C1 = 0.044715
F32 = jnp.float32
BF16 = jnp.bfloat16
NQ = 4
LEAD = 3
DIRECT = 0
TILE = 512
PLAN = ('own0 own1 own2 hop0 own3 hop1 own4 hop2 own5 last0 hop3 own6 last1 use0 hop4 own7 last2 use1 hop5 last3 use2 hop6 last4 use3 hop7 last5 use4 last6 use5 last7 use6 use7')
VMEM_LIMIT = 62 * 2 ** 20
NT = (((1,), (1,)), ((), ()))
TN = (((0,), (0,)), ((), ()))


def _gelu(u):
    u2 = u * u
    t = jnp.tanh(u * (C0 + (C0 * C1) * u2))
    p = 0.5 + 0.5 * t
    return u * p, p + (u * (1.0 - t * t)) * (0.5 * C0 + (1.5 * C0 * C1) * u2)


def schedule(n):
    return [(w[:-1], int(w[-1])) for w in PLAN.split()]


def _forward_kernel(ntp, x, dy, w1, w2, xg_o, dyg_o, z_o, dz_o, r_o,
                    g, w1v, w2v, acc, dact, z, dz, part, sendb, recvb, rr,
                    lsem, wsem, osem, ssem, rsem, psem):
    nchip = ntp // 2
    rows, h = x.shape
    hc = h // NQ
    f = w1.shape[1]
    me = lax.axis_index('tp')
    c = lax.rem(me, 2)
    chip = me // 2
    partner = me + 1 - 2 * c
    right = lax.rem(chip + 1, nchip) * 2 + c
    left = lax.rem(chip + nchip - 1, nchip) * 2 + c
    opp = lax.rem(chip + 2, nchip) * 2 + c
    fsrc = left * (1 - c) + right * c
    fdst = right * (1 - c) + left * c
    flip = 1 - 2 * c

    def piece(q, dev):
        return g.at[q, pl.ds(pl.multiple_of(dev * rows, rows), rows), :]

    def rcopy(q, slot, dev, to):
        return pltpu.make_async_remote_copy(
            src_ref=piece(q, dev), dst_ref=piece(q, dev), send_sem=ssem.at[q, slot], recv_sem=rsem.at[q, slot],
            device_id={'tp': to}, device_id_type=pl.DeviceIdType.MESH)

    own = []
    for q in range(2 * NQ):
        src = x if q < NQ else dy
        cp = pltpu.make_async_copy(src.at[:, pl.ds((q % NQ) * hc, hc)], piece(q, me), lsem.at[q])
        cp.start()
        own.append(cp)
    wcp = []
    for q in range(NQ):
        cp = pltpu.make_async_copy(w1.at[pl.ds(q * hc, hc), :], w1v.at[pl.ds(q * hc, hc), :], wsem.at[q])
        cp.start()
        wcp.append(cp)
    for q in range(NQ):
        cp = pltpu.make_async_copy(w2.at[:, pl.ds(q * hc, hc)], w2v.at[q], wsem.at[NQ + q])
        cp.start()
        wcp.append(cp)

    barrier = pltpu.get_barrier_semaphore()
    for nb in (partner, right, left, opp):
        pl.semaphore_signal(barrier, inc=1, device_id={'tp': nb}, device_id_type=pl.DeviceIdType.MESH)
    pl.semaphore_wait(barrier, 4)

    started = []

    def send(q, slot, dev, to):
        cp = rcopy(q, slot, dev, to)
        cp.start()
        started.append(cp)

    def send_own(q):
        if q < 2 * NQ - DIRECT:
            own[q].wait()
        send(q, 0, me, right)
        send(q, 1, me, left)
        send(q, 3, me, partner)

    def send_far(q):
        own[q].wait()
        send(q, 2, me, opp)

    def hop(q):
        rcopy(q, 0, left, me + 0).wait_recv()
        rcopy(q, 1, right, me + 0).wait_recv()
        if q < 2 * NQ - DIRECT:
            send(q, 2, fsrc, fdst)
        send(q, 4, left, partner)
        send(q, 5, right, partner)

    def last(q):
        rcopy(q, 2, opp, me + 0).wait_recv()
        send(q, 6, opp, partner)

    def arrived(q):
        rcopy(q, 3, partner, me + 0).wait_recv()
        rcopy(q, 4, left + flip, me + 0).wait_recv()
        rcopy(q, 5, right + flip, me + 0).wait_recv()
        rcopy(q, 6, opp + flip, me + 0).wait_recv()

    def use(q):
        arrived(q)
        compute(q)


    outs = []

    def put(src, dst):
        cp = pltpu.make_async_copy(src, dst, osem.at[len(outs)])
        cp.start()
        outs.append(cp)

    def compute(q):
        wcp[q].wait()
        ends = (q + 1) % NQ == 0
        lo = 0
        while lo < f:
            wide = min(TILE, f - lo) if ends else f
            cols = pl.ds(lo, wide)
            lo += wide
            if q < NQ:
                p = jnp.dot(g[q], w1v[pl.ds(q * hc, hc), cols], preferred_element_type=F32)
            else:
                p = lax.dot_general(g[q], w2v[q - NQ, cols, :], NT, preferred_element_type=F32)
            if q % NQ:
                p += acc[:, cols]
            if q == NQ - 1:
                g0, g1 = _gelu(p.astype(BF16).astype(F32))
                z[:, cols] = g0.astype(BF16)
                dact[:, cols] = g1
            elif q == 2 * NQ - 1:
                dz[:, cols] = (p * dact[:, cols]).astype(BF16)
            else:
                acc[:, cols] = p
        put(g.at[q], (xg_o if q < NQ else dyg_o).at[q % NQ])
        if q == NQ - 1:
            put(z, z_o)

    def use(q):
        arrived(q)
        compute(q)


    outs = []

    def put(src, dst):
        cp = pltpu.make_async_copy(src, dst, osem.at[len(outs)])
        cp.start()
        outs.append(cp)

    def compute(q):
        wcp[q].wait()
        for i in range(f // 256):
            cols = pl.ds(i * 256, 256)
            if q < NQ:
                p = jnp.dot(g[q], w1v[pl.ds(q * hc, hc), cols], preferred_element_type=F32)
            else:
                p = lax.dot_general(g[q], w2v[q - NQ, cols, :], NT, preferred_element_type=F32)
            if q % NQ:
                p += acc[:, cols]
            if q == NQ - 1:
                g0, g1 = _gelu(p.astype(BF16).astype(F32))
                z[:, cols] = g0.astype(BF16)
                dact[:, cols] = g1
            elif q == 2 * NQ - 1:
                dz[:, cols] = (p * dact[:, cols]).astype(BF16)
            else:
                acc[:, cols] = p
        put(g.at[q], (xg_o if q < NQ else dyg_o).at[q % NQ])
        if q == NQ - 1:
            put(z, z_o)

    def use(q):
        arrived(q)
        compute(q)

    acts = {'own': send_own, 'far': send_far, 'hop': hop, 'last': last, 'use': use}
    for name, q in schedule(2 * NQ):
        acts[name](q)

    put(dz, dz_o)

    def pair(j):
        return pltpu.make_async_remote_copy(
            src_ref=sendb.at[j], dst_ref=recvb.at[j], send_sem=psem.at[0, j], recv_sem=psem.at[1, j],
            device_id={'tp': partner}, device_id_type=pl.DeviceIdType.MESH)

    def block(d, core):
        dest = d * 2 + core
        return pl.ds(pl.multiple_of(dest * rows, rows), rows)

    def combine(j):
        pair(j).wait_recv()
        cols = pl.ds(j * hc, hc)
        for d in range(nchip):
            s = part[j % 2, block(d, c), :] + recvb[j, d].astype(F32)
            rr[d, :, cols] = s.astype(BF16)

    for j in range(NQ):
        part[j % 2] = lax.dot_general(dz[...], w1v[pl.ds(j * hc, hc), :], NT, preferred_element_type=F32)
        for d in range(nchip):
            sendb[j, d] = part[j % 2, block(d, 1 - c), :].astype(BF16)
        cp = pair(j)
        cp.start()
        started.append(cp)
        if j > 0:
            combine(j - 1)
    combine(NQ - 1)
    put(rr, r_o)
    for cp in started:
        cp.wait_send()
    for cp in outs:
        cp.wait()


def _weight_grad_kernel(xg, dyg, z, dz, dw1, dw2, xa, dya, za, dza, b1, b2, isem, sem1, sem2):
    nq, t, hc = xg.shape
    f = z.shape[1]
    n1, n2 = b1.shape[0], b2.shape[0]
    t1, t2 = b1.shape[1], b2.shape[1]
    k1, k2 = nq * hc // t1, f // t2
    cz = pltpu.make_async_copy(z, za, isem.at[0])
    cy = [pltpu.make_async_copy(dyg.at[q], dya.at[q], isem.at[1 + q]) for q in range(nq)]
    cx = pltpu.make_async_copy(xg, xa, isem.at[1 + nq])
    cd = pltpu.make_async_copy(dz, dza, isem.at[2 + nq])
    for cp in [cz] + cy + [cd, cx]:
        cp.start()
    cz.wait()

    def out2(i):
        s = lax.rem(i, n2)
        return pltpu.make_async_copy(b2.at[s], dw2.at[pl.ds(pl.multiple_of(i * t2, t2), t2), :], sem2.at[s])

    def out1(i):
        s = lax.rem(i, n1)
        return pltpu.make_async_copy(b1.at[s], dw1.at[pl.ds(pl.multiple_of(i * t1, t1), t1), :], sem1.at[s])

    for q in range(nq):
        cy[q].wait()
        b2[0, :, pl.ds(q * hc, hc)] = lax.dot_general(za[:, :t2], dya[q], TN, preferred_element_type=F32)
    out2(0).start()

    @pl.loop(1, k2)
    def _(i):
        @pl.when(i >= n2)
        def _():
            out2(i - n2).wait()
        zt = za[:, pl.ds(pl.multiple_of(i * t2, t2), t2)]
        s = lax.rem(i, n2)
        for q in range(nq):
            b2[s, :, pl.ds(q * hc, hc)] = lax.dot_general(zt, dya[q], TN, preferred_element_type=F32)
        out2(i).start()

    cx.wait()
    cd.wait()
    per = hc // t1

    @pl.loop(0, k1)
    def _(i):
        @pl.when(i >= n1)
        def _():
            out1(i - n1).wait()
        xt = xa[i // per, :, pl.ds(pl.multiple_of(lax.rem(i, per) * t1, t1), t1)]
        b1[lax.rem(i, n1)] = lax.dot_general(xt, dza[...], TN, preferred_element_type=F32)
        out1(i).start()

    for i in range(max(0, k2 - n2), k2):
        out2(i).wait()
    for i in range(max(0, k1 - n1), k1):
        out1(i).wait()


def solution(mesh):
    ntp = mesh.shape['tp']
    nchip = ntp // 2
    any_spec = pl.BlockSpec(memory_space=pl.ANY)

    def body(x, dy, w1, w2):
        rows, h = x.shape
        f = w1.shape[1]
        t, hc = rows * ntp, h // NQ
        sds = jax.ShapeDtypeStruct
        dma = pltpu.SemaphoreType.DMA
        xg, dyg, z, dz, r = pl.pallas_call(
            functools.partial(_forward_kernel, ntp),
            name='gather_forward',
            out_shape=[sds((NQ, t, hc), BF16), sds((NQ, t, hc), BF16), sds((t, f), BF16), sds((t, f), BF16),
                       sds((nchip, rows, h), BF16)],
            in_specs=[any_spec] * 4,
            out_specs=[any_spec] * 5,
            scratch_shapes=[
                pltpu.VMEM((2 * NQ, t, hc), BF16),
                pltpu.VMEM((h, f), BF16),
                pltpu.VMEM((NQ, f, hc), BF16),
                pltpu.VMEM((t, f), F32),
                pltpu.VMEM((t, f), F32),
                pltpu.VMEM((t, f), BF16),
                pltpu.VMEM((t, f), BF16),
                pltpu.VMEM((2, t, hc), F32),
                pltpu.VMEM((NQ, nchip, rows, hc), BF16),
                pltpu.VMEM((NQ, nchip, rows, hc), BF16),
                pltpu.VMEM((nchip, rows, h), BF16),
                dma((2 * NQ,)), dma((2 * NQ,)), dma((2 * NQ + 3,)),
                dma((2 * NQ, 7)), dma((2 * NQ, 7)), dma((2, NQ)),
            ],
            compiler_params=pltpu.CompilerParams(
                collective_id=0, has_side_effects=True, vmem_limit_bytes=VMEM_LIMIT),
            cost_estimate=pl.CostEstimate(flops=6 * t * h * f, bytes_accessed=4 * h * f, transcendentals=t * f),
        )(x, dy, w1, w2)

        groups = [[2 * i + k for i in range(nchip)] for k in range(2)]
        r = lax.all_to_all(r, 'tp', 0, 0, axis_index_groups=groups, tiled=True)
        t1, t2 = 512, 256
        dw1, dw2 = pl.pallas_call(
            _weight_grad_kernel,
            name='weight_grads',
            out_shape=[sds((h, f), F32), sds((f, h), F32)],
            in_specs=[any_spec] * 4,
            out_specs=[any_spec] * 2,
            scratch_shapes=[
                pltpu.VMEM((NQ, t, hc), BF16),
                pltpu.VMEM((NQ, t, hc), BF16),
                pltpu.VMEM((t, f), BF16),
                pltpu.VMEM((t, f), BF16),
                pltpu.VMEM((4, t1, f), F32),
                pltpu.VMEM((4, t2, h), F32),
                dma((NQ + 3,)), dma((4,)), dma((4,)),
            ],
            compiler_params=pltpu.CompilerParams(vmem_limit_bytes=VMEM_LIMIT),
            cost_estimate=pl.CostEstimate(flops=4 * t * h * f, bytes_accessed=8 * h * f, transcendentals=0),
        )(xg, dyg, z, dz)
        dx = jnp.sum(r.astype(F32), axis=0).astype(BF16)
        return dx, dw1, dw2

    return jax.shard_map(
        body, mesh=mesh,
        in_specs=(P(('dp', 'tp'), None), P(('dp', 'tp'), None), P(None, 'tp'), P('tp', None)),
        out_specs=(P(('dp', 'tp'), None), P('dp', 'tp'), P(('dp', 'tp'), None)),
        check_vma=False)
```

```python
import functools
import math

import jax
import jax.numpy as jnp
from jax import lax
from jax.experimental import pallas as pl
from jax.experimental.pallas import tpu as pltpu
from jax.sharding import PartitionSpec as P

C0 = math.sqrt(2.0 / math.pi)
C1 = 0.044715
F32 = jnp.float32
BF16 = jnp.bfloat16
NP = 4
NW = 16
TILE = 896
XC = (2, 2, 2, 2)
YC = (2, 2, 2, 1, 1)
LEAD = 3
LA = 2
AR = 3
GIVE = 1
VMEM_LIMIT = 62 * 2 ** 20
NT = (((1,), (1,)), ((), ()))
TN = (((0,), (0,)), ((), ()))


def _gelu(u):
    u2 = u * u
    t = jnp.tanh(u * (C0 + (C0 * C1) * u2))
    p = 0.5 + 0.5 * t
    return u * p, p + (u * (1.0 - t * t)) * (0.5 * C0 + (1.5 * C0 * C1) * u2)


def _forward_kernel(ntp, x, dy, w1, w2, xg_o, dyg_o, z_o, dz_o, r_o,
                    xg, dyg, w1v, w2v, w1p, acc, dact, z, dz, dzp, part, rr,
                    lsem, wsem, osem, ssem, rsem, xsem, psem):
    nchip = ntp // 2
    rows, h = x.shape
    half = h // 2
    hp = half // NP
    hw = half // NW
    f = w1.shape[1]
    me = lax.axis_index('tp')
    c = lax.rem(me, 2)
    chip = me // 2
    partner = me + 1 - 2 * c
    right = lax.rem(chip + 1, nchip) * 2 + c
    left = lax.rem(chip + nchip - 1, nchip) * 2 + c
    opp = lax.rem(chip + 2, nchip) * 2 + c
    fsrc = left * (1 - c) + right * c
    fdst = right * (1 - c) + left * c
    flip = 1 - 2 * c
    chunks = []
    for src, buf, sizes in ((x, xg, XC), (dy, dyg, YC)):
        for k, n in enumerate(sizes):
            chunks.append((src, buf, pl.ds(sum(sizes[:k]) * (h // 8), n * (h // 8))))
    nx, nq = len(XC), len(chunks)

    def piece(q, dev):
        _, buf, cols = chunks[q]
        return buf.at[pl.ds(pl.multiple_of(dev * rows, rows), rows), cols]

    def rcopy(q, slot, dev, to):
        return pltpu.make_async_remote_copy(
            src_ref=piece(q, dev), dst_ref=piece(q, dev), send_sem=ssem.at[q, slot], recv_sem=rsem.at[q, slot],
            device_id={'tp': to}, device_id_type=pl.DeviceIdType.MESH)

    own, wcp = [], []
    for q, (src, buf, cols) in enumerate(chunks):
        cp = pltpu.make_async_copy(src.at[:, cols], piece(q, me), lsem.at[q])
        cp.start()
        own.append(cp)
    for q, (src, buf, cols) in enumerate(chunks):
        wr, wb = (w1.at[cols, :], w1v.at[cols, :]) if q < nx else (w2.at[:, cols], w2v.at[:, cols])
        cp = pltpu.make_async_copy(wr, wb, wsem.at[q])
        cp.start()
        wcp.append(cp)

    barrier = pltpu.get_barrier_semaphore()
    for nb in (partner, right, left):
        pl.semaphore_signal(barrier, inc=1, device_id={'tp': nb}, device_id_type=pl.DeviceIdType.MESH)
    pl.semaphore_wait(barrier, 3)

    started = []

    def send(q, slot, dev, to):
        cp = rcopy(q, slot, dev, to)
        cp.start()
        started.append(cp)

    def send_own(q):
        own[q].wait()
        send(q, 0, me, right)
        send(q, 1, me, left)
        send(q, 3, me, partner)

    def hop(q):
        rcopy(q, 0, left, me + 0).wait_recv()
        rcopy(q, 1, right, me + 0).wait_recv()
        send(q, 2, fsrc, fdst)
        send(q, 4, left, partner)
        send(q, 5, right, partner)

    def last(q):
        rcopy(q, 2, opp, me + 0).wait_recv()
        send(q, 6, opp, partner)

    def arrived(q):
        rcopy(q, 3, partner, me + 0).wait_recv()
        rcopy(q, 4, left + flip, me + 0).wait_recv()
        rcopy(q, 5, right + flip, me + 0).wait_recv()
        rcopy(q, 6, opp + flip, me + 0).wait_recv()

    outs = []

    def put(src, dst):
        cp = pltpu.make_async_copy(src, dst, osem.at[len(outs)])
        cp.start()
        outs.append(cp)

    def weights(i):
        src = pl.ds(pl.multiple_of((1 - c) * half + i * hw, hw), hw)
        return pltpu.make_async_remote_copy(
            src_ref=w1v.at[src, :], dst_ref=w1p.at[pl.ds(i * hw, hw), :],
            send_sem=xsem.at[0, i], recv_sem=xsem.at[1, i],
            device_id={'tp': partner}, device_id_type=pl.DeviceIdType.MESH)

    tiles = [(lo, min(TILE, f - lo)) for lo in range(0, f, TILE)]

    def swap(i):
        cols = pl.ds(*tiles[i])
        return pltpu.make_async_remote_copy(
            src_ref=dz.at[:, cols], dst_ref=dzp.at[:, cols], send_sem=psem.at[0, i], recv_sem=psem.at[1, i],
            device_id={'tp': partner}, device_id_type=pl.DeviceIdType.MESH)

    def begin(cp):
        cp.start()
        started.append(cp)

    def compute(q):
        _, buf, hcols = chunks[q]
        if q >= nx:
            wcp[q].wait()
        ends = q in (nx - 1, nq - 1)
        for i, (lo, wide) in enumerate(tiles if ends else [(0, f)]):
            cols = pl.ds(lo, wide)
            if q < nx:
                p = jnp.dot(buf[:, hcols], w1v[hcols, cols], preferred_element_type=F32)
            else:
                p = lax.dot_general(buf[:, hcols], w2v[cols, hcols], NT, preferred_element_type=F32)
            if q not in (0, nx):
                p += acc[:, cols]
            if q == nx - 1:
                g0, g1 = _gelu(p.astype(BF16).astype(F32))
                z[:, cols] = g0.astype(BF16)
                dact[:, cols] = g1
            elif q == nq - 1:
                dz[:, cols] = (p * dact[:, cols]).astype(BF16)
                begin(swap(i))
            else:
                acc[:, cols] = p
        if q == nx - 1:
            put(xg, xg_o)
            put(z, z_o)
        elif q == nq - 1:
            put(dyg, dyg_o)

    def use(q):
        arrived(q)
        compute(q)

    for q in range(min(LEAD, nq)):
        send_own(q)
    given = 0
    for s in range(nq + AR):
        if s < nq:
            hop(s)
            if s + LEAD < nq:
                send_own(s + LEAD)
        if 0 <= s - LA < nq:
            last(s - LA)
        if s == GIVE:
            for q in range(nx):
                wcp[q].wait()
        if GIVE <= s < nq:
            for i in range(given, NW * (s - GIVE + 1) // (nq - GIVE)):
                begin(weights(i))
                given += 1
        if 0 <= s - AR < nq:
            use(s - AR)

    put(dz, dz_o)
    for j in range(NP):
        rws = pl.ds(pl.multiple_of(c * half + j * hp, hp), hp)
        part[j] = lax.dot_general(dz[...], w1v[rws, :], NT, preferred_element_type=F32)
    for i in range(NW):
        weights(i).wait_recv()
    for i in range(len(tiles)):
        swap(i).wait_recv()
    for j in range(NP):
        p = lax.dot_general(dzp[...], w1p[pl.ds(j * hp, hp), :], NT, preferred_element_type=F32)
        cols = pl.ds(j * hp, hp)
        rr[:, cols] = (part[j] + p).astype(BF16)
        put(rr.at[:, cols], r_o.at[:, cols])
    for cp in started:
        cp.wait_send()
    for cp in outs:
        cp.wait()


def _weight_grad_kernel(xg, dyg, z, dz, dw1, dw2, xa, dya, za, dza, b1, b2, isem, sem1, sem2):
    t, h = xg.shape
    nq = 4
    hc = h // nq
    f = z.shape[1]
    n1, n2 = b1.shape[0], b2.shape[0]
    t1, t2 = b1.shape[1], b2.shape[1]
    k1, k2 = h // t1, f // t2
    cz = pltpu.make_async_copy(z, za, isem.at[0])
    cy = [pltpu.make_async_copy(dyg.at[:, pl.ds(q * hc, hc)], dya.at[:, pl.ds(q * hc, hc)], isem.at[1 + q]) for q in range(nq)]
    cx = pltpu.make_async_copy(xg, xa, isem.at[1 + nq])
    cd = pltpu.make_async_copy(dz, dza, isem.at[2 + nq])
    for cp in [cz] + cy + [cd, cx]:
        cp.start()
    cz.wait()

    def out2(i):
        s = lax.rem(i, n2)
        return pltpu.make_async_copy(b2.at[s], dw2.at[pl.ds(pl.multiple_of(i * t2, t2), t2), :], sem2.at[s])

    def out1(i):
        s = lax.rem(i, n1)
        return pltpu.make_async_copy(b1.at[s], dw1.at[pl.ds(pl.multiple_of(i * t1, t1), t1), :], sem1.at[s])

    for q in range(nq):
        cy[q].wait()
        b2[0, :, pl.ds(q * hc, hc)] = lax.dot_general(za[:, :t2], dya[:, pl.ds(q * hc, hc)], TN, preferred_element_type=F32)
    out2(0).start()

    @pl.loop(1, k2)
    def _(i):
        @pl.when(i >= n2)
        def _():
            out2(i - n2).wait()
        zt = za[:, pl.ds(pl.multiple_of(i * t2, t2), t2)]
        s = lax.rem(i, n2)
        for q in range(nq):
            b2[s, :, pl.ds(q * hc, hc)] = lax.dot_general(zt, dya[:, pl.ds(q * hc, hc)], TN, preferred_element_type=F32)
        out2(i).start()

    cx.wait()
    cd.wait()

    @pl.loop(0, k1)
    def _(i):
        @pl.when(i >= n1)
        def _():
            out1(i - n1).wait()
        xt = xa[:, pl.ds(pl.multiple_of(i * t1, t1), t1)]
        b1[lax.rem(i, n1)] = lax.dot_general(xt, dza[...], TN, preferred_element_type=F32)
        out1(i).start()

    for i in range(max(0, k2 - n2), k2):
        out2(i).wait()
    for i in range(max(0, k1 - n1), k1):
        out1(i).wait()


def solution(mesh):
    ntp = mesh.shape['tp']
    nchip = ntp // 2
    any_spec = pl.BlockSpec(memory_space=pl.ANY)

    def body(x, dy, w1, w2):
        rows, h = x.shape
        f = w1.shape[1]
        t, half = rows * ntp, h // 2
        nt = -(-f // TILE)
        nq = len(XC) + len(YC)
        sds = jax.ShapeDtypeStruct
        dma = pltpu.SemaphoreType.DMA
        xg, dyg, z, dz, r = pl.pallas_call(
            functools.partial(_forward_kernel, ntp),
            name='gather_forward',
            out_shape=[sds((t, h), BF16), sds((t, h), BF16), sds((t, f), BF16), sds((t, f), BF16),
                       sds((t, half), BF16)],
            in_specs=[any_spec] * 4,
            out_specs=[any_spec] * 5,
            scratch_shapes=[
                pltpu.VMEM((t, h), BF16),
                pltpu.VMEM((t, h), BF16),
                pltpu.VMEM((h, f), BF16),
                pltpu.VMEM((f, h), BF16),
                pltpu.VMEM((half, f), BF16),
                pltpu.VMEM((t, f), F32),
                pltpu.VMEM((t, f), F32),
                pltpu.VMEM((t, f), BF16),
                pltpu.VMEM((t, f), BF16),
                pltpu.VMEM((t, f), BF16),
                pltpu.VMEM((NP, t, half // NP), F32),
                pltpu.VMEM((t, half), BF16),
                dma((nq,)), dma((nq,)), dma((4 + NP,)),
                dma((nq, 7)), dma((nq, 7)), dma((2, NW)), dma((2, nt)),
            ],
            compiler_params=pltpu.CompilerParams(
                collective_id=0, has_side_effects=True, vmem_limit_bytes=VMEM_LIMIT),
            cost_estimate=pl.CostEstimate(flops=6 * t * h * f, bytes_accessed=4 * h * f, transcendentals=t * f),
        )(x, dy, w1, w2)

        r = lax.all_to_all(r.reshape(ntp, rows, half), 'tp', 0, 0, tiled=True)
        t1, t2 = 512, 256
        dw1, dw2 = pl.pallas_call(
            _weight_grad_kernel,
            name='weight_grads',
            out_shape=[sds((h, f), F32), sds((f, h), F32)],
            in_specs=[any_spec] * 4,
            out_specs=[any_spec] * 2,
            scratch_shapes=[
                pltpu.VMEM((t, h), BF16),
                pltpu.VMEM((t, h), BF16),
                pltpu.VMEM((t, f), BF16),
                pltpu.VMEM((t, f), BF16),
                pltpu.VMEM((4, t1, f), F32),
                pltpu.VMEM((4, t2, h), F32),
                dma((7,)), dma((4,)), dma((4,)),
            ],
            compiler_params=pltpu.CompilerParams(vmem_limit_bytes=VMEM_LIMIT),
            cost_estimate=pl.CostEstimate(flops=4 * t * h * f, bytes_accessed=8 * h * f, transcendentals=0),
        )(xg, dyg, z, dz)
        r = r.astype(F32)
        dx = jnp.concatenate([sum(r[2 * i + k] for i in range(nchip)) for k in range(2)], axis=1).astype(BF16)
        return dx, dw1, dw2

    return jax.shard_map(
        body, mesh=mesh,
        in_specs=(P(('dp', 'tp'), None), P(('dp', 'tp'), None), P(None, 'tp'), P('tp', None)),
        out_specs=(P(('dp', 'tp'), None), P('dp', 'tp'), P(('dp', 'tp'), None)),
        check_vma=False)
```

```python
import functools
import math

import jax
import jax.numpy as jnp
from jax import lax
from jax.experimental import pallas as pl
from jax.experimental.pallas import tpu as pltpu
from jax.sharding import PartitionSpec as P

C0 = math.sqrt(2.0 / math.pi)
C1 = 0.044715
F32 = jnp.float32
BF16 = jnp.bfloat16
NP = 4
NW = 8
TILE = 896
XC = (2, 2, 2, 2)
YC = (2, 2, 2, 1, 1)
LEAD = 3
LA = 2
AR = 3
GIVE = 1
VMEM_LIMIT = 62 * 2 ** 20
NT = (((1,), (1,)), ((), ()))
TN = (((0,), (0,)), ((), ()))


def _gelu(u):
    u2 = u * u
    t = jnp.tanh(u * (C0 + (C0 * C1) * u2))
    p = 0.5 + 0.5 * t
    return u * p, p + (u * (1.0 - t * t)) * (0.5 * C0 + (1.5 * C0 * C1) * u2)


def _forward_kernel(ntp, x, dy, w1, w2, xg_o, dyg_o, z_o, dz_o, r_o,
                    xg, dyg, w1v, w2v, w1p, acc, dact, z, dz, dzp, part, rr,
                    lsem, wsem, osem, ssem, rsem, xsem, psem):
    nchip = ntp // 2
    rows, h = x.shape
    half = h // 2
    hp = half // NP
    hw = half // NW
    f = w1.shape[1]
    me = lax.axis_index('tp')
    c = lax.rem(me, 2)
    chip = me // 2
    partner = me + 1 - 2 * c
    right = lax.rem(chip + 1, nchip) * 2 + c
    left = lax.rem(chip + nchip - 1, nchip) * 2 + c
    opp = lax.rem(chip + 2, nchip) * 2 + c
    fsrc = left * (1 - c) + right * c
    fdst = right * (1 - c) + left * c
    flip = 1 - 2 * c
    chunks = []
    for src, buf, sizes in ((x, xg, XC), (dy, dyg, YC)):
        for k, n in enumerate(sizes):
            chunks.append((src, buf, pl.ds(sum(sizes[:k]) * (h // 8), n * (h // 8))))
    nx, nq = len(XC), len(chunks)

    def piece(q, dev):
        _, buf, cols = chunks[q]
        return buf.at[pl.ds(pl.multiple_of(dev * rows, rows), rows), cols]

    def rcopy(q, slot, dev, to):
        return pltpu.make_async_remote_copy(
            src_ref=piece(q, dev), dst_ref=piece(q, dev), send_sem=ssem.at[q, slot], recv_sem=rsem.at[q, slot],
            device_id={'tp': to}, device_id_type=pl.DeviceIdType.MESH)

    own, wcp = [], []
    for q, (src, buf, cols) in enumerate(chunks):
        cp = pltpu.make_async_copy(src.at[:, cols], piece(q, me), lsem.at[q])
        cp.start()
        own.append(cp)
    for q, (src, buf, cols) in enumerate(chunks):
        wr, wb = (w1.at[cols, :], w1v.at[cols, :]) if q < nx else (w2.at[:, cols], w2v.at[:, cols])
        cp = pltpu.make_async_copy(wr, wb, wsem.at[q])
        cp.start()
        wcp.append(cp)

    barrier = pltpu.get_barrier_semaphore()
    for nb in (partner, right, left):
        pl.semaphore_signal(barrier, inc=1, device_id={'tp': nb}, device_id_type=pl.DeviceIdType.MESH)
    pl.semaphore_wait(barrier, 3)

    started = []

    def send(q, slot, dev, to):
        cp = rcopy(q, slot, dev, to)
        cp.start()
        started.append(cp)

    def send_own(q):
        own[q].wait()
        send(q, 0, me, right)
        send(q, 1, me, left)
        send(q, 3, me, partner)

    def hop(q):
        rcopy(q, 0, left, me + 0).wait_recv()
        rcopy(q, 1, right, me + 0).wait_recv()
        send(q, 2, fsrc, fdst)
        send(q, 4, left, partner)
        send(q, 5, right, partner)

    def last(q):
        rcopy(q, 2, opp, me + 0).wait_recv()
        send(q, 6, opp, partner)

    def arrived(q):
        rcopy(q, 3, partner, me + 0).wait_recv()
        rcopy(q, 4, left + flip, me + 0).wait_recv()
        rcopy(q, 5, right + flip, me + 0).wait_recv()
        rcopy(q, 6, opp + flip, me + 0).wait_recv()

    outs = []

    def put(src, dst):
        cp = pltpu.make_async_copy(src, dst, osem.at[len(outs)])
        cp.start()
        outs.append(cp)

    def weights(i):
        src = pl.ds(pl.multiple_of((1 - c) * half + i * hw, hw), hw)
        return pltpu.make_async_remote_copy(
            src_ref=w1v.at[src, :], dst_ref=w1p.at[pl.ds(i * hw, hw), :],
            send_sem=xsem.at[0, i], recv_sem=xsem.at[1, i],
            device_id={'tp': partner}, device_id_type=pl.DeviceIdType.MESH)

    tiles = [(lo, min(TILE, f - lo)) for lo in range(0, f, TILE)]

    def swap(i):
        cols = pl.ds(*tiles[i])
        return pltpu.make_async_remote_copy(
            src_ref=dz.at[:, cols], dst_ref=dzp.at[:, cols], send_sem=psem.at[0, i], recv_sem=psem.at[1, i],
            device_id={'tp': partner}, device_id_type=pl.DeviceIdType.MESH)

    def begin(cp):
        cp.start()
        started.append(cp)

    def compute(q):
        _, buf, hcols = chunks[q]
        if q >= nx:
            wcp[q].wait()
        ends = q in (nx - 1, nq - 1)
        for i, (lo, wide) in enumerate(tiles if ends else [(0, f)]):
            cols = pl.ds(lo, wide)
            if q < nx:
                p = jnp.dot(buf[:, hcols], w1v[hcols, cols], preferred_element_type=F32)
            else:
                p = lax.dot_general(buf[:, hcols], w2v[cols, hcols], NT, preferred_element_type=F32)
            if q not in (0, nx):
                p += acc[:, cols]
            if q == nx - 1:
                g0, g1 = _gelu(p.astype(BF16).astype(F32))
                z[:, cols] = g0.astype(BF16)
                dact[:, cols] = g1
            elif q == nq - 1:
                dz[:, cols] = (p * dact[:, cols]).astype(BF16)
                begin(swap(i))
            else:
                acc[:, cols] = p
        if q == nx - 1:
            put(xg, xg_o)
            put(z, z_o)
        elif q == nq - 1:
            put(dyg, dyg_o)

    def use(q):
        arrived(q)
        compute(q)

    for q in range(min(LEAD, nq)):
        send_own(q)
    given = 0
    for s in range(nq + AR):
        if s < nq:
            hop(s)
            if s + LEAD < nq:
                send_own(s + LEAD)
        if 0 <= s - LA < nq:
            last(s - LA)
        if s == GIVE:
            for q in range(nx):
                wcp[q].wait()
        if GIVE <= s < nq:
            for i in range(given, NW * (s - GIVE + 1) // (nq - GIVE)):
                begin(weights(i))
                given += 1
        if 0 <= s - AR < nq:
            use(s - AR)

    put(dz, dz_o)
    for j in range(NP):
        rws = pl.ds(pl.multiple_of(c * half + j * hp, hp), hp)
        part[j] = lax.dot_general(dz[...], w1v[rws, :], NT, preferred_element_type=F32)
    for i in range(NW):
        weights(i).wait_recv()
    for i in range(len(tiles)):
        swap(i).wait_recv()
    for j in range(NP):
        p = lax.dot_general(dzp[...], w1p[pl.ds(j * hp, hp), :], NT, preferred_element_type=F32)
        cols = pl.ds(j * hp, hp)
        rr[:, cols] = (part[j] + p).astype(BF16)
        put(rr.at[:, cols], r_o.at[:, cols])
    for cp in started:
        cp.wait_send()
    for cp in outs:
        cp.wait()


def _weight_grad_kernel(xg, dyg, z, dz, dw1, dw2, xa, dya, za, dza, b1, b2, isem, sem1, sem2):
    t, h = xg.shape
    nq = 4
    hc = h // nq
    f = z.shape[1]
    n1, n2 = b1.shape[0], b2.shape[0]
    t1, t2 = b1.shape[1], b2.shape[1]
    k1, k2 = h // t1, f // t2
    cz = pltpu.make_async_copy(z, za, isem.at[0])
    cy = [pltpu.make_async_copy(dyg.at[:, pl.ds(q * hc, hc)], dya.at[:, pl.ds(q * hc, hc)], isem.at[1 + q]) for q in range(nq)]
    cx = pltpu.make_async_copy(xg, xa, isem.at[1 + nq])
    cd = pltpu.make_async_copy(dz, dza, isem.at[2 + nq])
    for cp in [cz] + cy:
        cp.start()
    cz.wait()

    def out2(i):
        s = lax.rem(i, n2)
        return pltpu.make_async_copy(b2.at[s], dw2.at[pl.ds(pl.multiple_of(i * t2, t2), t2), :], sem2.at[s])

    def out1(i):
        s = lax.rem(i, n1)
        return pltpu.make_async_copy(b1.at[s], dw1.at[pl.ds(pl.multiple_of(i * t1, t1), t1), :], sem1.at[s])

    for q in range(nq):
        cy[q].wait()
        if q == 2:
            cd.start()
            cx.start()
        b2[0, :, pl.ds(q * hc, hc)] = lax.dot_general(za[:, :t2], dya[:, pl.ds(q * hc, hc)], TN, preferred_element_type=F32)
    out2(0).start()

    @pl.loop(1, k2)
    def _(i):
        @pl.when(i >= n2)
        def _():
            out2(i - n2).wait()
        zt = za[:, pl.ds(pl.multiple_of(i * t2, t2), t2)]
        s = lax.rem(i, n2)
        for q in range(nq):
            b2[s, :, pl.ds(q * hc, hc)] = lax.dot_general(zt, dya[:, pl.ds(q * hc, hc)], TN, preferred_element_type=F32)
        out2(i).start()

    cx.wait()
    cd.wait()

    @pl.loop(0, k1)
    def _(i):
        @pl.when(i >= n1)
        def _():
            out1(i - n1).wait()
        xt = xa[:, pl.ds(pl.multiple_of(i * t1, t1), t1)]
        b1[lax.rem(i, n1)] = lax.dot_general(xt, dza[...], TN, preferred_element_type=F32)
        out1(i).start()

    for i in range(max(0, k2 - n2), k2):
        out2(i).wait()
    for i in range(max(0, k1 - n1), k1):
        out1(i).wait()


def solution(mesh):
    ntp = mesh.shape['tp']
    nchip = ntp // 2
    any_spec = pl.BlockSpec(memory_space=pl.ANY)

    def body(x, dy, w1, w2):
        rows, h = x.shape
        f = w1.shape[1]
        t, half = rows * ntp, h // 2
        nt = -(-f // TILE)
        nq = len(XC) + len(YC)
        sds = jax.ShapeDtypeStruct
        dma = pltpu.SemaphoreType.DMA
        xg, dyg, z, dz, r = pl.pallas_call(
            functools.partial(_forward_kernel, ntp),
            name='gather_forward',
            out_shape=[sds((t, h), BF16), sds((t, h), BF16), sds((t, f), BF16), sds((t, f), BF16),
                       sds((t, half), BF16)],
            in_specs=[any_spec] * 4,
            out_specs=[any_spec] * 5,
            scratch_shapes=[
                pltpu.VMEM((t, h), BF16),
                pltpu.VMEM((t, h), BF16),
                pltpu.VMEM((h, f), BF16),
                pltpu.VMEM((f, h), BF16),
                pltpu.VMEM((half, f), BF16),
                pltpu.VMEM((t, f), F32),
                pltpu.VMEM((t, f), F32),
                pltpu.VMEM((t, f), BF16),
                pltpu.VMEM((t, f), BF16),
                pltpu.VMEM((t, f), BF16),
                pltpu.VMEM((NP, t, half // NP), F32),
                pltpu.VMEM((t, half), BF16),
                dma((nq,)), dma((nq,)), dma((4 + NP,)),
                dma((nq, 7)), dma((nq, 7)), dma((2, NW)), dma((2, nt)),
            ],
            compiler_params=pltpu.CompilerParams(
                collective_id=0, has_side_effects=True, vmem_limit_bytes=VMEM_LIMIT),
            cost_estimate=pl.CostEstimate(flops=6 * t * h * f, bytes_accessed=4 * h * f, transcendentals=t * f),
        )(x, dy, w1, w2)

        r = lax.all_to_all(r.reshape(ntp, rows, half), 'tp', 0, 0, tiled=True)
        t1, t2 = 256, 128
        dw1, dw2 = pl.pallas_call(
            _weight_grad_kernel,
            name='weight_grads',
            out_shape=[sds((h, f), F32), sds((f, h), F32)],
            in_specs=[any_spec] * 4,
            out_specs=[any_spec] * 2,
            scratch_shapes=[
                pltpu.VMEM((t, h), BF16),
                pltpu.VMEM((t, h), BF16),
                pltpu.VMEM((t, f), BF16),
                pltpu.VMEM((t, f), BF16),
                pltpu.VMEM((8, t1, f), F32),
                pltpu.VMEM((8, t2, h), F32),
                dma((7,)), dma((8,)), dma((8,)),
            ],
            compiler_params=pltpu.CompilerParams(vmem_limit_bytes=VMEM_LIMIT),
            cost_estimate=pl.CostEstimate(flops=4 * t * h * f, bytes_accessed=8 * h * f, transcendentals=0),
        )(xg, dyg, z, dz)
        r = r.reshape(nchip, 2, rows, half)
        dx = jnp.sum(jnp.concatenate([r[:, 0], r[:, 1]], axis=2).astype(F32), axis=0).astype(BF16)
        return dx, dw1, dw2

    return jax.shard_map(
        body, mesh=mesh,
        in_specs=(P(('dp', 'tp'), None), P(('dp', 'tp'), None), P(None, 'tp'), P('tp', None)),
        out_specs=(P(('dp', 'tp'), None), P('dp', 'tp'), P(('dp', 'tp'), None)),
        check_vma=False)
```

```python
import functools
import math

import jax
import jax.numpy as jnp
from jax import lax
from jax.experimental import pallas as pl
from jax.experimental.pallas import tpu as pltpu
from jax.sharding import PartitionSpec as P

C0 = math.sqrt(2.0 / math.pi)
C1 = 0.044715
F32 = jnp.float32
BF16 = jnp.bfloat16
NP = 4
NW = 8
TILE = 896
XC = (2, 2, 2, 2)
YC = (2, 2, 2, 1, 1)
LEAD = 3
LA = 2
AR = 3
GIVE = 1
VMEM_LIMIT = 62 * 2 ** 20
NT = (((1,), (1,)), ((), ()))
TN = (((0,), (0,)), ((), ()))


def _gelu(u):
    u2 = u * u
    t = jnp.tanh(u * (C0 + (C0 * C1) * u2))
    p = 0.5 + 0.5 * t
    return u * p, p + (u * (1.0 - t * t)) * (0.5 * C0 + (1.5 * C0 * C1) * u2)


def _forward_kernel(ntp, x, dy, w1, w2, xg_o, dyg_o, z_o, dz_o, r_o,
                    xg, dyg, w1v, w2v, w1p, acc, dact, z, dz, dzp, part, rr,
                    lsem, wsem, osem, ssem, rsem, xsem, psem):
    nchip = ntp // 2
    rows, h = x.shape
    half = h // 2
    hp = half // NP
    hw = half // NW
    f = w1.shape[1]
    me = lax.axis_index('tp')
    c = lax.rem(me, 2)
    chip = me // 2
    partner = me + 1 - 2 * c
    right = lax.rem(chip + 1, nchip) * 2 + c
    left = lax.rem(chip + nchip - 1, nchip) * 2 + c
    opp = lax.rem(chip + 2, nchip) * 2 + c
    fsrc = left * (1 - c) + right * c
    fdst = right * (1 - c) + left * c
    flip = 1 - 2 * c
    chunks = []
    for src, buf, sizes in ((x, xg, XC), (dy, dyg, YC)):
        for k, n in enumerate(sizes):
            chunks.append((src, buf, pl.ds(sum(sizes[:k]) * (h // 8), n * (h // 8))))
    nx, nq = len(XC), len(chunks)

    def piece(q, dev):
        _, buf, cols = chunks[q]
        return buf.at[pl.ds(pl.multiple_of(dev * rows, rows), rows), cols]

    def rcopy(q, slot, dev, to):
        return pltpu.make_async_remote_copy(
            src_ref=piece(q, dev), dst_ref=piece(q, dev), send_sem=ssem.at[q, slot], recv_sem=rsem.at[q, slot],
            device_id={'tp': to}, device_id_type=pl.DeviceIdType.MESH)

    own, wcp = [], []
    for q, (src, buf, cols) in enumerate(chunks):
        cp = pltpu.make_async_copy(src.at[:, cols], piece(q, me), lsem.at[q])
        cp.start()
        own.append(cp)
    for q, (src, buf, cols) in enumerate(chunks):
        wr, wb = (w1.at[cols, :], w1v.at[cols, :]) if q < nx else (w2.at[:, cols], w2v.at[:, cols])
        cp = pltpu.make_async_copy(wr, wb, wsem.at[q])
        if q < nx:
            cp.start()
        wcp.append(cp)

    barrier = pltpu.get_barrier_semaphore()
    for nb in (partner, right, left):
        pl.semaphore_signal(barrier, inc=1, device_id={'tp': nb}, device_id_type=pl.DeviceIdType.MESH)
    pl.semaphore_wait(barrier, 3)

    started = []

    def send(q, slot, dev, to):
        cp = rcopy(q, slot, dev, to)
        cp.start()
        started.append(cp)

    def send_own(q):
        own[q].wait()
        send(q, 0, me, right)
        send(q, 1, me, left)
        send(q, 3, me, partner)

    def hop(q):
        rcopy(q, 0, left, me + 0).wait_recv()
        rcopy(q, 1, right, me + 0).wait_recv()
        send(q, 2, fsrc, fdst)
        send(q, 4, left, partner)
        send(q, 5, right, partner)

    def last(q):
        rcopy(q, 2, opp, me + 0).wait_recv()
        send(q, 6, opp, partner)

    def arrived(q):
        rcopy(q, 3, partner, me + 0).wait_recv()
        rcopy(q, 4, left + flip, me + 0).wait_recv()
        rcopy(q, 5, right + flip, me + 0).wait_recv()
        rcopy(q, 6, opp + flip, me + 0).wait_recv()

    outs = []

    def put(src, dst):
        cp = pltpu.make_async_copy(src, dst, osem.at[len(outs)])
        cp.start()
        outs.append(cp)

    def weights(i):
        src = pl.ds(pl.multiple_of((1 - c) * half + i * hw, hw), hw)
        return pltpu.make_async_remote_copy(
            src_ref=w1v.at[src, :], dst_ref=w1p.at[pl.ds(i * hw, hw), :],
            send_sem=xsem.at[0, i], recv_sem=xsem.at[1, i],
            device_id={'tp': partner}, device_id_type=pl.DeviceIdType.MESH)

    tiles = [(lo, min(TILE, f - lo)) for lo in range(0, f, TILE)]

    def swap(i):
        cols = pl.ds(*tiles[i])
        return pltpu.make_async_remote_copy(
            src_ref=dz.at[:, cols], dst_ref=dzp.at[:, cols], send_sem=psem.at[0, i], recv_sem=psem.at[1, i],
            device_id={'tp': partner}, device_id_type=pl.DeviceIdType.MESH)

    def begin(cp):
        cp.start()
        started.append(cp)

    def compute(q):
        _, buf, hcols = chunks[q]
        if q >= nx:
            wcp[q].wait()
        ends = q in (nx - 1, nq - 1)
        for i, (lo, wide) in enumerate(tiles if ends else [(0, f)]):
            cols = pl.ds(lo, wide)
            if q < nx:
                p = jnp.dot(buf[:, hcols], w1v[hcols, cols], preferred_element_type=F32)
            else:
                p = lax.dot_general(buf[:, hcols], w2v[cols, hcols], NT, preferred_element_type=F32)
            if q not in (0, nx):
                p += acc[:, cols]
            if q == nx - 1:
                g0, g1 = _gelu(p.astype(BF16).astype(F32))
                z[:, cols] = g0.astype(BF16)
                dact[:, cols] = g1
            elif q == nq - 1:
                dz[:, cols] = (p * dact[:, cols]).astype(BF16)
                begin(swap(i))
            else:
                acc[:, cols] = p
        if q == nx - 1:
            put(xg, xg_o)
            put(z, z_o)
        elif q == nq - 1:
            put(dyg, dyg_o)

    def use(q):
        arrived(q)
        compute(q)

    for q in range(min(LEAD, nq)):
        send_own(q)
    given = 0
    for s in range(nq + AR):
        if s < nq:
            hop(s)
            if s + LEAD < nq:
                send_own(s + LEAD)
        if 0 <= s - LA < nq:
            last(s - LA)
        if s == GIVE:
            for q in range(nx):
                wcp[q].wait()
            for q in range(nx, nq):
                wcp[q].start()
        if GIVE <= s < nq:
            for i in range(given, NW * (s - GIVE + 1) // (nq - GIVE)):
                begin(weights(i))
                given += 1
        if 0 <= s - AR < nq:
            use(s - AR)

    put(dz, dz_o)
    for j in range(NP):
        rws = pl.ds(pl.multiple_of(c * half + j * hp, hp), hp)
        part[j] = lax.dot_general(dz[...], w1v[rws, :], NT, preferred_element_type=F32)
    for i in range(NW):
        weights(i).wait_recv()
    for i in range(len(tiles)):
        swap(i).wait_recv()
    for j in range(NP):
        p = lax.dot_general(dzp[...], w1p[pl.ds(j * hp, hp), :], NT, preferred_element_type=F32)
        cols = pl.ds(j * hp, hp)
        rr[:, cols] = (part[j] + p).astype(BF16)
        put(rr.at[:, cols], r_o.at[:, cols])
    for cp in started:
        cp.wait_send()
    for cp in outs:
        cp.wait()


def _weight_grad_kernel(xg, dyg, z, dz, dw1, dw2, xa, dya, za, dza, b1, b2, isem, sem1, sem2):
    t, h = xg.shape
    nq = 4
    hc = h // nq
    f = z.shape[1]
    n1, n2 = b1.shape[0], b2.shape[0]
    t1, t2 = b1.shape[1], b2.shape[1]
    k1, k2 = h // t1, f // t2
    cz = pltpu.make_async_copy(z, za, isem.at[0])
    cy = [pltpu.make_async_copy(dyg.at[:, pl.ds(q * hc, hc)], dya.at[:, pl.ds(q * hc, hc)], isem.at[1 + q]) for q in range(nq)]
    cx = pltpu.make_async_copy(xg, xa, isem.at[1 + nq])
    cd = pltpu.make_async_copy(dz, dza, isem.at[2 + nq])
    for cp in [cz] + cy:
        cp.start()
    cz.wait()

    def out2(i):
        s = lax.rem(i, n2)
        return pltpu.make_async_copy(b2.at[s], dw2.at[pl.ds(pl.multiple_of(i * t2, t2), t2), :], sem2.at[s])

    def out1(i):
        s = lax.rem(i, n1)
        return pltpu.make_async_copy(b1.at[s], dw1.at[pl.ds(pl.multiple_of(i * t1, t1), t1), :], sem1.at[s])

    for q in range(nq):
        cy[q].wait()
        if q == 2:
            cd.start()
            cx.start()
        b2[0, :, pl.ds(q * hc, hc)] = lax.dot_general(za[:, :t2], dya[:, pl.ds(q * hc, hc)], TN, preferred_element_type=F32)
    out2(0).start()

    @pl.loop(1, k2)
    def _(i):
        @pl.when(i >= n2)
        def _():
            out2(i - n2).wait()
        zt = za[:, pl.ds(pl.multiple_of(i * t2, t2), t2)]
        s = lax.rem(i, n2)
        for q in range(nq):
            b2[s, :, pl.ds(q * hc, hc)] = lax.dot_general(zt, dya[:, pl.ds(q * hc, hc)], TN, preferred_element_type=F32)
        out2(i).start()

    cx.wait()
    cd.wait()

    @pl.loop(0, k1)
    def _(i):
        @pl.when(i >= n1)
        def _():
            out1(i - n1).wait()
        xt = xa[:, pl.ds(pl.multiple_of(i * t1, t1), t1)]
        b1[lax.rem(i, n1)] = lax.dot_general(xt, dza[...], TN, preferred_element_type=F32)
        out1(i).start()

    for i in range(max(0, k2 - n2), k2):
        out2(i).wait()
    for i in range(max(0, k1 - n1), k1):
        out1(i).wait()


def solution(mesh):
    ntp = mesh.shape['tp']
    nchip = ntp // 2
    any_spec = pl.BlockSpec(memory_space=pl.ANY)

    def body(x, dy, w1, w2):
        rows, h = x.shape
        f = w1.shape[1]
        t, half = rows * ntp, h // 2
        nt = -(-f // TILE)
        nq = len(XC) + len(YC)
        sds = jax.ShapeDtypeStruct
        dma = pltpu.SemaphoreType.DMA
        xg, dyg, z, dz, r = pl.pallas_call(
            functools.partial(_forward_kernel, ntp),
            name='gather_forward',
            out_shape=[sds((t, h), BF16), sds((t, h), BF16), sds((t, f), BF16), sds((t, f), BF16),
                       sds((t, half), BF16)],
            in_specs=[any_spec] * 4,
            out_specs=[any_spec] * 5,
            scratch_shapes=[
                pltpu.VMEM((t, h), BF16),
                pltpu.VMEM((t, h), BF16),
                pltpu.VMEM((h, f), BF16),
                pltpu.VMEM((f, h), BF16),
                pltpu.VMEM((half, f), BF16),
                pltpu.VMEM((t, f), F32),
                pltpu.VMEM((t, f), F32),
                pltpu.VMEM((t, f), BF16),
                pltpu.VMEM((t, f), BF16),
                pltpu.VMEM((t, f), BF16),
                pltpu.VMEM((NP, t, half // NP), F32),
                pltpu.VMEM((t, half), BF16),
                dma((nq,)), dma((nq,)), dma((4 + NP,)),
                dma((nq, 7)), dma((nq, 7)), dma((2, NW)), dma((2, nt)),
            ],
            compiler_params=pltpu.CompilerParams(
                collective_id=0, has_side_effects=True, vmem_limit_bytes=VMEM_LIMIT),
            cost_estimate=pl.CostEstimate(flops=6 * t * h * f, bytes_accessed=4 * h * f, transcendentals=t * f),
        )(x, dy, w1, w2)

        r = lax.all_to_all(r.reshape(ntp, rows, half), 'tp', 0, 0, tiled=True)
        t1, t2 = 256, 128
        dw1, dw2 = pl.pallas_call(
            _weight_grad_kernel,
            name='weight_grads',
            out_shape=[sds((h, f), F32), sds((f, h), F32)],
            in_specs=[any_spec] * 4,
            out_specs=[any_spec] * 2,
            scratch_shapes=[
                pltpu.VMEM((t, h), BF16),
                pltpu.VMEM((t, h), BF16),
                pltpu.VMEM((t, f), BF16),
                pltpu.VMEM((t, f), BF16),
                pltpu.VMEM((8, t1, f), F32),
                pltpu.VMEM((8, t2, h), F32),
                dma((7,)), dma((8,)), dma((8,)),
            ],
            compiler_params=pltpu.CompilerParams(vmem_limit_bytes=VMEM_LIMIT),
            cost_estimate=pl.CostEstimate(flops=4 * t * h * f, bytes_accessed=8 * h * f, transcendentals=0),
        )(xg, dyg, z, dz)
        r = r.reshape(nchip, 2, rows, half)
        dx = jnp.sum(jnp.concatenate([r[:, 0], r[:, 1]], axis=2).astype(F32), axis=0).astype(BF16)
        return dx, dw1, dw2

    return jax.shard_map(
        body, mesh=mesh,
        in_specs=(P(('dp', 'tp'), None), P(('dp', 'tp'), None), P(None, 'tp'), P('tp', None)),
        out_specs=(P(('dp', 'tp'), None), P('dp', 'tp'), P(('dp', 'tp'), None)),
        check_vma=False)
```
